32 devices in a mesh: ty: 4 (over x, core), tx: 8 (over z, y).
Axes of the slice: x: 2, y: 2, z: 4, core: 2. Of those that a mesh axis runs over, the one named last changes fastest.
Arguments:
- potential_warmth: float32 [16, 512, 4096], P(None, ('ty', 'tx')), may hold values from -2 to 30
- saltiness_field: float32 [16, 512, 4096], P(None, ('ty', 'tx')), may hold values from 30 to 38
- ocean_tier_tally: int32 [512, 4096], P(('ty', 'tx')), may hold values from 0 to 16, as said below
Outputs:
- buoyancy_anomaly: float32 [16, 512, 4096], P(None, 'ty', 'tx')
- laplacian: float32 [16, 512, 4096], P(None, 'ty', 'tx')
The draws below stay inside these ranges and needn't reach their ends.
Inputs may be any that keep to these rules, and one draw needn't show every extreme that they name: `ocean_tier_tally`: columns with 0 are land; the tile of rows 0 .. 127 and columns 0 .. 511 is land in every draw, and other whole tiles of land occur. Within the rows of one device and the columns of one tile, at most 6144 columns are ocean, and some such block has exactly 6144.
All inputs are finite; a program needn't handle non-finite values.
Results may differ from the reference program's by a relative error of at most 0.00002.
Values sent between devices are 32-bit elements; how exact they have to be, the bound alone decides.
A program may use at most 128 MiB of HBM per device.

```python
import jax
import jax.numpy as jnp

SOUNDING_TIERS = 16
CJ = 128
CI = 512
MESH_PARALLELS = 512
MESH_MERIDIANS = 4096
BAND = 16
OCEAN_COLS = 6144


def draw_ocean_tier_tally(key, part):
    first_key, second_key, third_key, fourth_key, fifth_key = jax.random.split(key, 5)
    tile_rows = MESH_PARALLELS // CJ
    tile_cols = MESH_MERIDIANS // CI
    groups = MESH_PARALLELS // BAND
    land_tiles = jax.random.randint(first_key, (tile_rows, tile_cols), 0, 4) == 0
    land_tiles = land_tiles.at[0, 0].set(True)
    land_tiles = land_tiles.at[tile_rows - 1, tile_cols - 1].set(False)
    scores = jax.random.randint(fourth_key, (groups, BAND, tile_cols, CI), 0, 1 << 30)
    scores = jnp.transpose(scores, (0, 2, 1, 3)).reshape(groups, tile_cols, BAND * CI)
    ranks = jnp.argsort(jnp.argsort(scores, axis=2, stable=True), axis=2, stable=True)
    counts = jax.random.randint(fifth_key, (groups, tile_cols), OCEAN_COLS // 2, OCEAN_COLS + 1)
    counts = counts.at[groups - 1, tile_cols - 1].set(OCEAN_COLS)
    ocean_cols = ranks < counts[:, :, None]
    ocean_cols = jnp.transpose(ocean_cols.reshape(groups, tile_cols, BAND, CI), (0, 2, 1, 3)).reshape(MESH_PARALLELS, MESH_MERIDIANS)
    levels_drawn = jax.random.randint(second_key, (MESH_PARALLELS, MESH_MERIDIANS), 1, SOUNDING_TIERS + 1)
    full_depth = jax.random.randint(third_key, (MESH_PARALLELS, MESH_MERIDIANS), 0, 2)
    levels_drawn = jnp.where(full_depth == 1, SOUNDING_TIERS, levels_drawn)
    land_cells = jnp.repeat(jnp.repeat(land_tiles, CJ, 0), CI, 1)
    keep = jnp.logical_and(ocean_cols, jnp.logical_not(land_cells))
    return jnp.where(keep, levels_drawn, 0).astype(jnp.int32)


def shard_levels(key, shape, cuts, least, largest):
    factor_of, own = 1.0, jax.random.fold_in(key, 6)
    for dim, shards_of in cuts:
        draws = jnp.exp(jax.random.uniform(jax.random.fold_in(own, dim), (shards_of,), jnp.float32, least / len(cuts), largest / len(cuts)))
        factor_of = factor_of * jnp.repeat(draws, shape[dim] // shards_of).reshape([-1 if axis == dim else 1 for axis in range(len(shape))])
    return factor_of


def setup_inputs(seed: int = 0) -> dict:
    key_of = jax.random.split(jax.random.key(seed), 4)
    return {
        "potential_warmth": jnp.clip(-2.0 + 32.0 * jax.random.uniform(key_of[0], (SOUNDING_TIERS, MESH_PARALLELS, MESH_MERIDIANS), jnp.float32) ** shard_levels(key_of[0], (SOUNDING_TIERS, MESH_PARALLELS, MESH_MERIDIANS), ((1, 32),), -0.2, 0.2), -2.0, 30.0),
        "saltiness_field": jnp.clip(30.0 + 8.0 * jax.random.uniform(key_of[1], (SOUNDING_TIERS, MESH_PARALLELS, MESH_MERIDIANS), jnp.float32) ** shard_levels(key_of[1], (SOUNDING_TIERS, MESH_PARALLELS, MESH_MERIDIANS), ((1, 32),), -0.2, 0.2), 30.0, 38.0),
        "ocean_tier_tally": draw_ocean_tier_tally(jax.random.fold_in(key_of[3], 71), 0),
    }


therm_coef = 0.16550
haline_coef = 0.76554
cabbel_coef = 0.059520
haline_second = 0.00054914
thermo_press = 0.00014970
haline_press = 0.000011090
cross_coef = 0.0024341


def ocean_properties(potential_warmth, saltiness_field, wet_indicator, sounding_tiers_list):
    heat_properties = potential_warmth - 10.0
    haline = saltiness_field - 35.0
    height = sounding_tiers_list[:, None, None]
    anomaly = -therm_coef * (1.0 + 0.5 * cabbel_coef * heat_properties + thermo_press * height) * heat_properties
    anomaly = anomaly + haline_coef * (1.0 - 0.5 * haline_second * haline - haline_press * height) * haline
    anomaly = anomaly - cross_coef * heat_properties * haline
    return wet_indicator * anomaly


def reference(potential_warmth, saltiness_field, ocean_tier_tally):
    level_index = jnp.arange(SOUNDING_TIERS, dtype=jnp.int32)
    wet_indicator = (level_index[:, None, None] < ocean_tier_tally[None]).astype(jnp.float32)
    sounding_tiers_list = 5.0 + 10.0 * jnp.arange(SOUNDING_TIERS, dtype=jnp.float32)
    buoyancy_anomaly = ocean_properties(potential_warmth, saltiness_field, wet_indicator, sounding_tiers_list)
    north_density = jnp.concatenate([buoyancy_anomaly[:, 1:, :], buoyancy_anomaly[:, -1:, ::-1]], 1)
    north_ocean = jnp.concatenate([wet_indicator[:, 1:, :], wet_indicator[:, -1:, ::-1]], 1)
    south_density = jnp.concatenate([jnp.zeros_like(buoyancy_anomaly[:, :1]), buoyancy_anomaly[:, :-1]], 1)
    south_ocean = jnp.concatenate([jnp.zeros_like(wet_indicator[:, :1]), wet_indicator[:, :-1]], 1)
    east_density = jnp.roll(buoyancy_anomaly, -1, 2)
    east_ocean = jnp.roll(wet_indicator, -1, 2)
    west_density = jnp.roll(buoyancy_anomaly, 1, 2)
    west_ocean = jnp.roll(wet_indicator, 1, 2)
    laplacian = north_ocean * (north_density - buoyancy_anomaly) + south_ocean * (south_density - buoyancy_anomaly)
    laplacian = laplacian + east_ocean * (east_density - buoyancy_anomaly) + west_ocean * (west_density - buoyancy_anomaly)
    return buoyancy_anomaly, wet_indicator * laplacian
```

```python
import functools

import jax
import jax.numpy as jnp
from jax import lax
from jax.experimental import pallas as pl
from jax.experimental.pallas import tpu as pltpu
from jax.sharding import PartitionSpec as P

therm_coef = 0.1655
haline_coef = 0.76554
cabbel_coef = 0.05952
haline_second = 0.00054914
thermo_press = 0.0001497
haline_press = 1.109e-05
cross_coef = 0.0024341

MESH = pl.DeviceIdType.MESH
LANES = 128
MIB = 1 << 20


def density(warmth, salt, wet, height):
    heat = warmth - 10.0
    haline = salt - 35.0
    anomaly = -therm_coef * (1.0 + 0.5 * cabbel_coef * heat + thermo_press * height) * heat
    anomaly = anomaly + haline_coef * (1.0 - 0.5 * haline_second * haline - haline_press * height) * haline
    anomaly = anomaly - cross_coef * heat * haline
    return jnp.where(wet, anomaly, 0.0)


def exchange(
    ny, nx, groups,
    warmth_ref, salt_ref, tally_ref,
    tile_ref, bottom_ref, sides_ref, north_ref, south_ref, fold_ref,
    warmth, salt, tally, dens, pack, slab, slab_bottom, low, high,
    load_sem, send_sem, recv_sem, bsend_sem, brecv_sem, psend_sem, precv_sem, own_sem, slab_sem, hsend_sem, hrecv_sem,
):
    y, x = lax.axis_index("ty"), lax.axis_index("tx")
    levels, band, width = dens.shape
    wide = width // nx
    depth = levels // groups
    up, down = lax.rem(y + 1, ny), lax.rem(y + ny - 1, ny)
    last = y == ny - 1

    loads = []
    for g in range(groups):
        part = pl.ds(g * depth, depth)
        pair = [
            pltpu.make_async_copy(warmth_ref.at[part], warmth.at[part], load_sem.at[2 * g]),
            pltpu.make_async_copy(salt_ref.at[part], salt.at[part], load_sem.at[2 * g + 1]),
        ]
        if g == 0:
            load_tally = pltpu.make_async_copy(tally_ref, tally, load_sem.at[2 * groups])
            load_tally.start()
        for copy in pair:
            copy.start()
        loads.append(pair)

    barrier = pltpu.get_barrier_semaphore()
    for m in range(1, nx):
        pl.semaphore_signal(barrier, inc=1, device_id=(y, x ^ m), device_id_type=MESH)
    for other in (up, down):
        pl.semaphore_signal(barrier, inc=1, device_id=(other, x), device_id_type=MESH)

    def columns(t):
        return pl.ds(pl.multiple_of(t * wide, LANES), wide)

    def rows(t):
        return pl.ds(pl.multiple_of(t * band, 8), band)

    mine = rows(x)

    def bottom_copy(m):
        t = x ^ m
        return pltpu.make_async_remote_copy(
            src_ref=tally_ref.at[:, columns(t)], dst_ref=bottom_ref.at[mine],
            send_sem=bsend_sem.at[m], recv_sem=brecv_sem.at[x], device_id=(y, t), device_id_type=MESH)

    def dens_copy(g, m):
        t = x ^ m
        part = pl.ds(g * depth, depth)
        return pltpu.make_async_remote_copy(
            src_ref=dens.at[part, :, columns(t)], dst_ref=tile_ref.at[part, mine],
            send_sem=send_sem.at[g, m], recv_sem=recv_sem.at[g, x], device_id=(y, t), device_id_type=MESH)

    def pack_copy(m):
        t = x ^ m
        return pltpu.make_async_remote_copy(
            src_ref=pack.at[t], dst_ref=sides_ref.at[mine],
            send_sem=psend_sem.at[m], recv_sem=precv_sem.at[x], device_id=(y, t), device_id_type=MESH)

    own = [
        pltpu.make_async_copy(dens.at[:, :, columns(x)], tile_ref.at[:, mine], own_sem.at[0]),
        pltpu.make_async_copy(tally_ref.at[:, columns(x)], bottom_ref.at[mine], own_sem.at[1]),
        pltpu.make_async_copy(pack.at[x], sides_ref.at[mine], own_sem.at[2]),
    ]
    far = [m for m in range(nx - 1, 0, -1) if m >= nx // 2]
    near = [m for m in range(nx - 1, 0, -1) if m < nx // 2]

    pl.semaphore_wait(barrier, nx - 1 + 2)
    for m in far + near:
        bottom_copy(m).start()
    own[1].start()
    load_tally.wait()

    lane = lax.broadcasted_iota(jnp.int32, (band, LANES), 1)

    def fill(t, _):
        before = lax.rem(t + nx - 1, nx)
        after = lax.rem(t + 1, nx)
        left = tally[:, pl.ds(pl.multiple_of(before * wide + wide - LANES, LANES), LANES)].astype(jnp.float32)
        right = tally[:, pl.ds(pl.multiple_of(after * wide, LANES), LANES)].astype(jnp.float32)
        cells = jnp.where(lane == 2 * levels, jnp.broadcast_to(left[:, LANES - 1:], (band, LANES)), 0.0)
        cells = jnp.where(lane == 2 * levels + 1, jnp.broadcast_to(right[:, :1], (band, LANES)), cells)
        pack[t] = cells
        return 0

    lax.fori_loop(0, nx, fill, 0)

    def level(k, _):
        height = 5.0 + 10.0 * k.astype(jnp.float32)

        def block(t, _):
            cols = columns(t)
            value = density(warmth[k, :, cols], salt[k, :, cols], k < tally[:, cols], height)
            dens[k, :, cols] = value
            after = lax.rem(t + 1, nx)
            before = lax.rem(t + nx - 1, nx)
            pack[after] = jnp.where(lane == k, jnp.broadcast_to(value[:, wide - 1:], (band, LANES)), pack[after])
            pack[before] = jnp.where(lane == levels + k, jnp.broadcast_to(value[:, :1], (band, LANES)), pack[before])
            return 0

        lax.fori_loop(0, nx, block, 0)
        return 0

    for g in range(groups):
        for copy in loads[g]:
            copy.wait()
        lax.fori_loop(g * depth, (g + 1) * depth, level, 0)
        for m in far:
            dens_copy(g, m).start()
    own[0].start()
    own[2].start()
    for g in range(groups):
        for m in near:
            dens_copy(g, m).start()
    for m in far + near:
        pack_copy(m).start()

    own[0].wait()
    own[1].wait()

    def arrive(s):
        @pl.when(x != s)
        def _():
            pltpu.make_async_copy(bottom_ref.at[rows(s)], bottom_ref.at[rows(s)], brecv_sem.at[s]).wait()
            for g in range(groups):
                part = tile_ref.at[pl.ds(g * depth, depth), rows(s)]
                pltpu.make_async_copy(part, part, recv_sem.at[g, s]).wait()

    arrive(0)
    arrive(nx - 1)
    top = nx * band - 8
    slabs = [
        pltpu.make_async_copy(tile_ref.at[:, pl.ds(0, 8)], slab.at[0], slab_sem.at[0]),
        pltpu.make_async_copy(tile_ref.at[:, pl.ds(top, 8)], slab.at[1], slab_sem.at[1]),
        pltpu.make_async_copy(bottom_ref.at[pl.ds(0, 8)], slab_bottom.at[0], slab_sem.at[2]),
        pltpu.make_async_copy(bottom_ref.at[pl.ds(top, 8)], slab_bottom.at[1], slab_sem.at[3]),
    ]
    for copy in slabs:
        copy.start()
    for copy in slabs:
        copy.wait()
    for k in range(levels):
        low[k:k + 1, :] = slab[0, k, 0:1, :]
        high[k:k + 1, :] = slab[1, k, 7:8, :]
    low[levels:, :] = jnp.broadcast_to(slab_bottom[0, 0:1, :].astype(jnp.float32), (8, wide))
    high[levels:, :] = jnp.broadcast_to(slab_bottom[1, 7:8, :].astype(jnp.float32), (8, wide))

    def halo(index, src, dst, target):
        return pltpu.make_async_remote_copy(
            src_ref=src, dst_ref=dst, send_sem=hsend_sem.at[index], recv_sem=hrecv_sem.at[index],
            device_id=target, device_id_type=MESH)

    to_south = halo(0, low, north_ref, (down, x))
    to_north = halo(1, high, south_ref, (up, x))
    across = halo(2, high, fold_ref, (y, x ^ (nx - 1)))
    to_south.start()
    to_north.start()

    @pl.when(last)
    def _():
        across.start()

    for s in range(1, nx - 1):
        arrive(s)
    for s in range(nx):
        @pl.when(x != s)
        def _():
            pltpu.make_async_copy(sides_ref.at[rows(s)], sides_ref.at[rows(s)], precv_sem.at[s]).wait()
    own[2].wait()
    to_south.wait()
    to_north.wait()

    @pl.when(last)
    def _():
        across.wait()

    for m in far + near:
        bottom_copy(m).wait_send()
        pack_copy(m).wait_send()
        for g in range(groups):
            dens_copy(g, m).wait_send()


def stencil(
    ny, levels, per,
    tile_ref, bottom_ref, sides_ref, north_ref, south_ref, fold_ref,
    dens_ref, lap_ref,
    north, south, bottoms,
):
    y = lax.axis_index("ty")
    tall, wide = bottom_ref.shape
    row = lax.broadcasted_iota(jnp.int32, (tall, wide), 0)
    col = lax.broadcasted_iota(jnp.int32, (tall, wide), 1)
    side_lane = lax.broadcasted_iota(jnp.int32, sides_ref.shape, 1)

    def side(index):
        return jnp.sum(jnp.where(side_lane == index, sides_ref[...], 0.0), axis=1, keepdims=True)

    def around(cells, top, base, left, right):
        above = jnp.where(row == tall - 1, top, pltpu.roll(cells, tall - 1, 0))
        below = jnp.where(row == 0, base, pltpu.roll(cells, 1, 0))
        east = jnp.where(col == wide - 1, right, pltpu.roll(cells, wide - 1, 1))
        west = jnp.where(col == 0, left, pltpu.roll(cells, 1, 1))
        return above, below, east, west

    @pl.when(pl.program_id(0) == 0)
    def _():
        mirror = fold_ref[...]
        lane = lax.broadcasted_iota(jnp.int32, mirror.shape, 1)
        bit = 1
        while bit < wide:
            mirror = jnp.where((lane & bit) != 0, pltpu.roll(mirror, bit, 1), pltpu.roll(mirror, wide - bit, 1))
            bit *= 2
        north[...] = jnp.where(y == ny - 1, mirror, north_ref[...])
        south[...] = jnp.where(y == 0, 0.0, south_ref[...])
        own = bottom_ref[...].astype(jnp.float32)
        near = around(own, north[levels:levels + 1, :], south[levels:levels + 1, :], side(2 * levels), side(2 * levels + 1))
        bottoms[0] = own
        for index in range(4):
            bottoms[index + 1] = near[index]

    for j in range(per):
        k = pl.program_id(0) * per + j
        number = k.astype(jnp.float32)
        cells = tile_ref[j]
        near = around(cells, north[pl.ds(k, 1), :], south[pl.ds(k, 1), :], side(k), side(levels + k))
        count = jnp.where(number < bottoms[1], 1.0, 0.0)
        for index in range(2, 5):
            count = count + jnp.where(number < bottoms[index], 1.0, 0.0)
        total = (near[0] + near[1]) + (near[2] + near[3]) - count * cells
        dens_ref[j] = cells
        lap_ref[j] = jnp.where(number < bottoms[0], total, 0.0)


def on_device(ny, nx, potential_warmth, saltiness_field, ocean_tier_tally):
    levels, band, width = potential_warmth.shape
    wide, tall = width // nx, band * nx
    groups = 4 if levels % 4 == 0 else 1
    hbm = pl.BlockSpec(memory_space=pl.ANY)
    f32, i32 = jnp.float32, jnp.int32
    edge = jax.ShapeDtypeStruct((levels + 8, wide), f32)
    dma = pltpu.SemaphoreType.DMA
    parts = pl.pallas_call(
        functools.partial(exchange, ny, nx, groups),
        out_shape=(
            jax.ShapeDtypeStruct((levels, tall, wide), f32),
            jax.ShapeDtypeStruct((tall, wide), i32),
            jax.ShapeDtypeStruct((tall, LANES), f32),
            edge, edge, edge,
        ),
        in_specs=[hbm] * 3,
        out_specs=(hbm,) * 6,
        scratch_shapes=[
            pltpu.VMEM((levels, band, width), f32),
            pltpu.VMEM((levels, band, width), f32),
            pltpu.VMEM((band, width), i32),
            pltpu.VMEM((levels, band, width), f32),
            pltpu.VMEM((nx, band, LANES), f32),
            pltpu.VMEM((2, levels, 8, wide), f32),
            pltpu.VMEM((2, 8, wide), i32),
            pltpu.VMEM((levels + 8, wide), f32),
            pltpu.VMEM((levels + 8, wide), f32),
            dma((2 * groups + 1,)),
            dma((groups, nx)), dma((groups, nx)),
            dma((nx,)), dma((nx,)), dma((nx,)), dma((nx,)),
            dma((3,)), dma((4,)), dma((3,)), dma((3,)),
        ],
        compiler_params=pltpu.CompilerParams(collective_id=0, has_side_effects=True, vmem_limit_bytes=24 * MIB),
        cost_estimate=pl.CostEstimate(flops=0, bytes_accessed=16 * levels * band * width, transcendentals=0),
        name="exchange",
    )(potential_warmth, saltiness_field, ocean_tier_tally)
    per = 2 if levels % 2 == 0 else 1
    block = pl.BlockSpec((per, tall, wide), lambda i: (i, 0, 0))
    whole = pl.BlockSpec(memory_space=pltpu.VMEM)
    out = jax.ShapeDtypeStruct((levels, tall, wide), f32)
    return pl.pallas_call(
        functools.partial(stencil, ny, levels, per),
        grid=(levels // per,),
        out_shape=(out, out),
        in_specs=[block] + [whole] * 5,
        out_specs=(block, block),
        scratch_shapes=[
            pltpu.VMEM((levels + 8, wide), f32),
            pltpu.VMEM((levels + 8, wide), f32),
            pltpu.VMEM((5, tall, wide), f32),
        ],
        compiler_params=pltpu.CompilerParams(vmem_limit_bytes=24 * MIB),
        name="stencil",
    )(*parts)


def solution(mesh):
    placed = (P(None, ("ty", "tx"), None), P(None, ("ty", "tx"), None), P(("ty", "tx"), None))
    return jax.shard_map(
        functools.partial(on_device, mesh.shape["ty"], mesh.shape["tx"]),
        mesh=mesh,
        in_specs=placed,
        out_specs=(P(None, "ty", "tx"), P(None, "ty", "tx")),
        check_vma=False,
    )
```

```python
import functools

import jax
import jax.numpy as jnp
from jax import lax
from jax.experimental import pallas as pl
from jax.experimental.pallas import tpu as pltpu
from jax.sharding import PartitionSpec as P

therm_coef = 0.1655
haline_coef = 0.76554
cabbel_coef = 0.05952
haline_second = 0.00054914
thermo_press = 0.0001497
haline_press = 1.109e-05
cross_coef = 0.0024341

MESH = pl.DeviceIdType.MESH
LANES = 128
MIB = 1 << 20
roll = pltpu.roll
GRANT = 32 * MIB


def density(warmth, salt, wet, height):
    heat = warmth - 10.0
    haline = salt - 35.0
    anomaly = -therm_coef * (1.0 + 0.5 * cabbel_coef * heat + thermo_press * height) * heat
    anomaly = anomaly + haline_coef * (1.0 - 0.5 * haline_second * haline - haline_press * height) * haline
    anomaly = anomaly - cross_coef * heat * haline
    return jnp.where(wet, anomaly, 0.0)


def swapped(cells, j):
    lane = lax.broadcasted_iota(jnp.int32, (8, LANES), 1)
    sub = lax.broadcasted_iota(jnp.int32, (8, LANES), 0)
    if j >= 10:
        return [cells[v ^ (1 << (j - 10))] for v in range(len(cells))]
    axis, size, place, bit = (1, LANES, lane, 1 << j) if j < 7 else (0, 8, sub, 1 << (j - 7))
    if 2 * bit == size:
        return [roll(c, bit, axis) for c in cells]
    upper = (place & bit) != 0
    return [jnp.where(upper, roll(c, bit, axis), roll(c, size - bit, axis)) for c in cells]


def stages_of(count):
    return 10 + count.bit_length() - 1


def routes(wet):
    count = len(wet)
    flags = jnp.concatenate([jnp.where(w, 1.0, 0.0) for w in wet], axis=0)
    height = flags.shape[0]
    upper = lax.broadcasted_iota(jnp.int32, (LANES, LANES), 0) <= lax.broadcasted_iota(jnp.int32, (LANES, LANES), 1)
    lower = lax.broadcasted_iota(jnp.int32, (height, height), 1) < lax.broadcasted_iota(jnp.int32, (height, height), 0)
    upto = jnp.dot(flags, jnp.where(upper, 1.0, 0.0), preferred_element_type=jnp.float32)
    totals = jnp.broadcast_to(upto[:, LANES - 1:], (height, LANES))
    before = jnp.dot(jnp.where(lower, 1.0, 0.0), totals, preferred_element_type=jnp.float32)
    rank = jnp.where(flags > 0.0, (before + upto - flags).astype(jnp.int32), -1)
    ranks = [rank[8 * v:8 * v + 8] for v in range(count)]
    lane = lax.broadcasted_iota(jnp.int32, (8, LANES), 1)
    sub = lax.broadcasted_iota(jnp.int32, (8, LANES), 0)
    packing = [jnp.zeros((8, LANES), jnp.int32)] * count
    unpacking = [jnp.zeros((8, LANES), jnp.int32)] * count
    for j in range(stages_of(count)):
        others = swapped(ranks, j)
        following = []
        for v in range(count):
            here = (lane >> j) & 1 if j < 7 else (sub >> (j - 7)) & 1 if j < 10 else (v >> (j - 10)) & 1
            mine, other = ranks[v], others[v]
            takes = jnp.where(other >= 0, ((other >> j) & 1) ^ here, 1) == 0
            stays = jnp.where(mine >= 0, ((mine >> j) & 1) ^ here, 1) == 0
            leaves = jnp.where(mine >= 0, ((mine >> j) & 1) ^ here, 0) == 1
            packing[v] = jnp.where(takes, packing[v] | (1 << j), packing[v])
            unpacking[v] = jnp.where(leaves, unpacking[v] | (1 << j), unpacking[v])
            following.append(jnp.where(takes, other, jnp.where(stays, mine, -1)))
        ranks = following
    return packing, unpacking


def moved(layers, masks, order):
    for j in order:
        takes = [(mask & (1 << j)) != 0 for mask in masks]
        layers = [
            [jnp.where(t, o, c) for t, o, c in zip(takes, swapped(cells, j), cells)] for cells in layers
        ]
    return layers


def pieces(block):
    tall, wide = block.shape
    return [
        block[r:r + 8, c:c + LANES] for r in range(0, tall, 8) for c in range(0, wide, LANES)
    ]


def exchange(
    ny, nx, groups,
    warmth_ref, salt_ref, tally_ref,
    tile_ref, bottom_ref, sides_ref, north_ref, south_ref, fold_ref,
    warmth, salt, tally, dens, pack, outbox, inbox, packing, unpacking, low, high,
    load_sem, send_sem, recv_sem, bsend_sem, brecv_sem, psend_sem, precv_sem, own_sem, hsend_sem, hrecv_sem,
):
    y, x = lax.axis_index("ty"), lax.axis_index("tx")
    levels, band, width = dens.shape
    wide = width // nx
    depth = levels // groups
    up, down = lax.rem(y + 1, ny), lax.rem(y + ny - 1, ny)
    last = y == ny - 1

    loads = []
    for g in range(groups):
        part = pl.ds(g * depth, depth)
        pair = [
            pltpu.make_async_copy(warmth_ref.at[part], warmth.at[part], load_sem.at[2 * g]),
            pltpu.make_async_copy(salt_ref.at[part], salt.at[part], load_sem.at[2 * g + 1]),
        ]
        if g == 0:
            load_tally = pltpu.make_async_copy(tally_ref, tally, load_sem.at[2 * groups])
            load_tally.start()
        for copy in pair:
            copy.start()
        loads.append(pair)

    barrier = pltpu.get_barrier_semaphore()
    for m in range(1, nx):
        pl.semaphore_signal(barrier, inc=1, device_id=(y, x ^ m), device_id_type=MESH)
    for other in (up, down):
        pl.semaphore_signal(barrier, inc=1, device_id=(other, x), device_id_type=MESH)

    def columns(t):
        return pl.ds(pl.multiple_of(t * wide, LANES), wide)

    def rows(t):
        return pl.ds(pl.multiple_of(t * band, 8), band)

    mine = rows(x)

    def bottom_copy(m):
        t = x ^ m
        return pltpu.make_async_remote_copy(
            src_ref=tally_ref.at[:, columns(t)], dst_ref=bottom_ref.at[mine],
            send_sem=bsend_sem.at[m], recv_sem=brecv_sem.at[x], device_id=(y, t), device_id_type=MESH)

    def dens_copy(g, m):
        t = x ^ m
        part = pl.ds(g * depth, depth)
        return pltpu.make_async_remote_copy(
            src_ref=outbox.at[t, part], dst_ref=inbox.at[x, part],
            send_sem=send_sem.at[g, m], recv_sem=recv_sem.at[g, x], device_id=(y, t), device_id_type=MESH)

    def pack_copy(m):
        t = x ^ m
        return pltpu.make_async_remote_copy(
            src_ref=pack.at[t], dst_ref=sides_ref.at[mine],
            send_sem=psend_sem.at[m], recv_sem=precv_sem.at[x], device_id=(y, t), device_id_type=MESH)

    own = [
        pltpu.make_async_copy(dens.at[:, :, columns(x)], tile_ref.at[:, mine], own_sem.at[0]),
        pltpu.make_async_copy(tally_ref.at[:, columns(x)], bottom_ref.at[mine], own_sem.at[1]),
        pltpu.make_async_copy(pack.at[x], sides_ref.at[mine], own_sem.at[2]),
    ]
    far = [m for m in range(nx - 1, 0, -1) if m >= nx // 2]
    near = [m for m in range(nx - 1, 0, -1) if m < nx // 2]

    pl.semaphore_wait(barrier, nx - 1 + 2)
    for m in far + near:
        bottom_copy(m).start()
    own[1].start()
    load_tally.wait()

    lane = lax.broadcasted_iota(jnp.int32, (band, LANES), 1)

    def fill(t, _):
        before = lax.rem(t + nx - 1, nx)
        after = lax.rem(t + 1, nx)
        left = tally[:, pl.ds(pl.multiple_of(before * wide + wide - LANES, LANES), LANES)].astype(jnp.float32)
        right = tally[:, pl.ds(pl.multiple_of(after * wide, LANES), LANES)].astype(jnp.float32)
        cells = jnp.where(lane == 2 * levels, jnp.broadcast_to(left[:, LANES - 1:], (band, LANES)), 0.0)
        cells = jnp.where(lane == 2 * levels + 1, jnp.broadcast_to(right[:, :1], (band, LANES)), cells)
        pack[t] = cells
        return 0

    count = band * wide // (8 * LANES)
    kept = outbox.shape[2] // 8
    stages = stages_of(count)

    def plan(m, _):
        t = x ^ m
        wet = [piece > 0 for piece in pieces(tally[:, columns(t)])]
        for v, mask in enumerate(routes(wet)[0]):
            packing[t, v] = mask
        return 0

    def gather(g, first):
        def block(i, _):
            t = x ^ (first - i)
            masks = [packing[t, v] for v in range(count)]
            for k0 in range(0, depth, 2):
                ks = [g * depth + k for k in range(k0, min(k0 + 2, depth))]
                layers = moved([pieces(dens[k, :, columns(t)]) for k in ks], masks, range(stages))
                for k, cells in zip(ks, layers):
                    for v in range(kept):
                        outbox[t, k, 8 * v:8 * v + 8, :] = cells[v]
            return 0
        return block

    lax.fori_loop(1, nx, plan, 0)

    def level(k, _):
        height = 5.0 + 10.0 * k.astype(jnp.float32)

        def block(t, _):
            cols = columns(t)
            value = density(warmth[k, :, cols], salt[k, :, cols], k < tally[:, cols], height)
            dens[k, :, cols] = value
            return 0

        lax.fori_loop(0, nx, block, 0)
        return 0

    for g in range(groups):
        for copy in loads[g]:
            copy.wait()
        lax.fori_loop(g * depth, (g + 1) * depth, level, 0)
        lax.fori_loop(0, len(far), gather(g, far[0]), 0)
        for m in far:
            dens_copy(g, m).start()
        lax.fori_loop(0, len(near), gather(g, near[0]), 0)
    lax.fori_loop(0, nx, fill, 0)

    def edges(t, _):
        before = lax.rem(t + nx - 1, nx)
        after = lax.rem(t + 1, nx)
        before_cols = pl.ds(pl.multiple_of(before * wide + wide - LANES, LANES), LANES)
        after_cols = pl.ds(pl.multiple_of(after * wide, LANES), LANES)
        cells = pack[t]
        for k in range(levels):
            left = jnp.broadcast_to(dens[k, :, before_cols][:, LANES - 1:], (band, LANES))
            right = jnp.broadcast_to(dens[k, :, after_cols][:, :1], (band, LANES))
            cells = jnp.where(lane == k, left, jnp.where(lane == levels + k, right, cells))
        pack[t] = cells
        return 0

    lax.fori_loop(0, nx, edges, 0)
    own[0].start()
    own[2].start()
    for g in range(groups):
        for m in near:
            dens_copy(g, m).start()
    for m in far + near:
        pack_copy(m).start()

    own[0].wait()
    own[1].wait()
    for m in far + near:
        bottom_copy(m).wait_send()
    for s in range(nx):
        @pl.when(x != s)
        def _():
            pltpu.make_async_copy(bottom_ref.at[rows(s)], bottom_ref.at[rows(s)], brecv_sem.at[s]).wait()

    def unplan(m, _):
        s = x ^ m
        wet = [piece > 0 for piece in pieces(bottom_ref[rows(s), :])]
        for v, mask in enumerate(routes(wet)[1]):
            unpacking[s, v] = mask
        return 0

    lax.fori_loop(1, nx, unplan, 0)

    def spread(first, number):
        def block(q, _):
            g, s = q // number, x ^ (first - q % number)
            part = inbox.at[s, pl.ds(g * depth, depth)]
            pltpu.make_async_copy(part, part, recv_sem.at[g, s]).wait()
            masks = [unpacking[s, v] for v in range(count)]
            blank = [jnp.zeros((8, LANES), jnp.float32)] * (count - kept)
            for k0 in range(0, depth, 2):
                ks = [g * depth + k for k in range(k0, min(k0 + 2, depth))]
                layers = [[inbox[s, k, 8 * v:8 * v + 8, :] for v in range(kept)] + blank for k in ks]
                layers = moved(layers, masks, range(stages - 1, -1, -1))
                for k, cells in zip(ks, layers):
                    for r in range(0, band, 8):
                        line = r // 8 * (wide // LANES)
                        value = jnp.concatenate(cells[line:line + wide // LANES], axis=1)
                        at = pl.ds(pl.multiple_of(s * band + r, 8), 8)
                        tile_ref[k, at, :] = jnp.where(k < bottom_ref[at, :], value, 0.0)
            return 0
        return block

    lax.fori_loop(0, groups * len(far), spread(far[0], len(far)), 0)
    lax.fori_loop(0, groups * len(near), spread(near[0], len(near)), 0)
    tall = nx * band
    for k in range(levels):
        low[k:k + 1, :] = tile_ref[k, 0:1, :]
        high[k:k + 1, :] = tile_ref[k, tall - 1:tall, :]
    low[levels:, :] = jnp.broadcast_to(bottom_ref[0:1, :].astype(jnp.float32), (8, wide))
    high[levels:, :] = jnp.broadcast_to(bottom_ref[tall - 1:tall, :].astype(jnp.float32), (8, wide))

    def halo(index, src, dst, target):
        return pltpu.make_async_remote_copy(
            src_ref=src, dst_ref=dst, send_sem=hsend_sem.at[index], recv_sem=hrecv_sem.at[index],
            device_id=target, device_id_type=MESH)

    to_south = halo(0, low, north_ref, (down, x))
    to_north = halo(1, high, south_ref, (up, x))
    across = halo(2, high, fold_ref, (y, x ^ (nx - 1)))
    to_south.start()
    to_north.start()

    @pl.when(last)
    def _():
        across.start()

    for s in range(nx):
        @pl.when(x != s)
        def _():
            pltpu.make_async_copy(sides_ref.at[rows(s)], sides_ref.at[rows(s)], precv_sem.at[s]).wait()
    own[2].wait()
    to_south.wait()
    to_north.wait()

    @pl.when(last)
    def _():
        across.wait()

    for m in far + near:
        pack_copy(m).wait_send()
        for g in range(groups):
            dens_copy(g, m).wait_send()


def stencil(
    ny, levels, per,
    tile_ref, bottom_ref, sides_ref, north_ref, south_ref, fold_ref,
    dens_ref, lap_ref,
    north, south, bottoms,
):
    y = lax.axis_index("ty")
    tall, wide = bottom_ref.shape
    row = lax.broadcasted_iota(jnp.int32, (tall, wide), 0)
    col = lax.broadcasted_iota(jnp.int32, (tall, wide), 1)
    side_lane = lax.broadcasted_iota(jnp.int32, sides_ref.shape, 1)

    def side(index):
        return jnp.sum(jnp.where(side_lane == index, sides_ref[...], 0.0), axis=1, keepdims=True)

    def around(cells, top, base, left, right):
        above = jnp.where(row == tall - 1, top, pltpu.roll(cells, tall - 1, 0))
        below = jnp.where(row == 0, base, pltpu.roll(cells, 1, 0))
        east = jnp.where(col == wide - 1, right, pltpu.roll(cells, wide - 1, 1))
        west = jnp.where(col == 0, left, pltpu.roll(cells, 1, 1))
        return above, below, east, west

    @pl.when(pl.program_id(0) == 0)
    def _():
        mirror = fold_ref[...]
        lane = lax.broadcasted_iota(jnp.int32, mirror.shape, 1)
        bit = 1
        while bit < wide:
            mirror = jnp.where((lane & bit) != 0, pltpu.roll(mirror, bit, 1), pltpu.roll(mirror, wide - bit, 1))
            bit *= 2
        north[...] = jnp.where(y == ny - 1, mirror, north_ref[...])
        south[...] = jnp.where(y == 0, 0.0, south_ref[...])
        own = bottom_ref[...].astype(jnp.float32)
        near = around(own, north[levels:levels + 1, :], south[levels:levels + 1, :], side(2 * levels), side(2 * levels + 1))
        bottoms[0] = own
        for index in range(4):
            bottoms[index + 1] = near[index]

    for j in range(per):
        k = pl.program_id(0) * per + j
        number = k.astype(jnp.float32)
        cells = tile_ref[j]
        near = around(cells, north[pl.ds(k, 1), :], south[pl.ds(k, 1), :], side(k), side(levels + k))
        count = jnp.where(number < bottoms[1], 1.0, 0.0)
        for index in range(2, 5):
            count = count + jnp.where(number < bottoms[index], 1.0, 0.0)
        total = (near[0] + near[1]) + (near[2] + near[3]) - count * cells
        dens_ref[j] = cells
        lap_ref[j] = jnp.where(number < bottoms[0], total, 0.0)


def on_device(ny, nx, potential_warmth, saltiness_field, ocean_tier_tally):
    levels, band, width = potential_warmth.shape
    wide, tall = width // nx, band * nx
    groups = 4 if levels % 4 == 0 else 1
    count = band * wide // (8 * LANES)
    kept = 8 * (3 * count // 4)
    hbm = pl.BlockSpec(memory_space=pltpu.HBM)
    vmem = pl.BlockSpec(memory_space=pltpu.VMEM)
    f32, i32 = jnp.float32, jnp.int32
    edge = jax.ShapeDtypeStruct((levels + 8, wide), f32)
    dma = pltpu.SemaphoreType.DMA
    parts = pl.pallas_call(
        functools.partial(exchange, ny, nx, groups),
        out_shape=(
            jax.ShapeDtypeStruct((levels, tall, wide), f32),
            jax.ShapeDtypeStruct((tall, wide), i32),
            jax.ShapeDtypeStruct((tall, LANES), f32),
            edge, edge, edge,
        ),
        in_specs=[hbm] * 3,
        out_specs=(vmem,) * 6,
        scratch_shapes=[
            pltpu.VMEM((levels, band, width), f32),
            pltpu.VMEM((levels, band, width), f32),
            pltpu.VMEM((band, width), i32),
            pltpu.VMEM((levels, band, width), f32),
            pltpu.VMEM((nx, band, LANES), f32),
            pltpu.VMEM((nx, levels, kept, LANES), f32),
            pltpu.VMEM((nx, levels, kept, LANES), f32),
            pltpu.VMEM((nx, count, 8, LANES), i32),
            pltpu.VMEM((nx, count, 8, LANES), i32),
            pltpu.VMEM((levels + 8, wide), f32),
            pltpu.VMEM((levels + 8, wide), f32),
            dma((2 * groups + 1,)),
            dma((groups, nx)), dma((groups, nx)),
            dma((nx,)), dma((nx,)), dma((nx,)), dma((nx,)),
            dma((3,)), dma((3,)), dma((3,)),
        ],
        compiler_params=pltpu.CompilerParams(collective_id=0, has_side_effects=True, vmem_limit_bytes=GRANT),
        cost_estimate=pl.CostEstimate(flops=0, bytes_accessed=16 * levels * band * width, transcendentals=0),
        name="exchange",
    )(potential_warmth, saltiness_field, ocean_tier_tally)
    per = 2 if levels % 2 == 0 else 1
    block = pl.BlockSpec((per, tall, wide), lambda i: (i, 0, 0))
    whole = pl.BlockSpec(memory_space=pltpu.VMEM)
    out = jax.ShapeDtypeStruct((levels, tall, wide), f32)
    return pl.pallas_call(
        functools.partial(stencil, ny, levels, per),
        grid=(levels // per,),
        out_shape=(out, out),
        in_specs=[block] + [whole] * 5,
        out_specs=(block, block),
        scratch_shapes=[
            pltpu.VMEM((levels + 8, wide), f32),
            pltpu.VMEM((levels + 8, wide), f32),
            pltpu.VMEM((5, tall, wide), f32),
        ],
        compiler_params=pltpu.CompilerParams(vmem_limit_bytes=24 * MIB),
        name="stencil",
    )(*parts)


def solution(mesh):
    placed = (P(None, ("ty", "tx"), None), P(None, ("ty", "tx"), None), P(("ty", "tx"), None))
    return jax.shard_map(
        functools.partial(on_device, mesh.shape["ty"], mesh.shape["tx"]),
        mesh=mesh,
        in_specs=placed,
        out_specs=(P(None, "ty", "tx"), P(None, "ty", "tx")),
        check_vma=False,
    )
```

```python
import functools

import jax
import jax.numpy as jnp
from jax import lax
from jax.experimental import pallas as pl
from jax.experimental.pallas import tpu as pltpu
from jax.sharding import PartitionSpec as P

therm_coef = 0.1655
haline_coef = 0.76554
cabbel_coef = 0.05952
haline_second = 0.00054914
thermo_press = 0.0001497
haline_press = 1.109e-05
cross_coef = 0.0024341

MESH = pl.DeviceIdType.MESH
LANES = 128
MIB = 1 << 20
roll = pltpu.roll
GRANT = 46 * MIB


def density(warmth, salt, wet, height):
    heat = warmth - 10.0
    haline = salt - 35.0
    anomaly = -therm_coef * (1.0 + 0.5 * cabbel_coef * heat + thermo_press * height) * heat
    anomaly = anomaly + haline_coef * (1.0 - 0.5 * haline_second * haline - haline_press * height) * haline
    anomaly = anomaly - cross_coef * heat * haline
    return jnp.where(wet, anomaly, 0.0)


def swapped(cells, j):
    lane = lax.broadcasted_iota(jnp.int32, (8, LANES), 1)
    sub = lax.broadcasted_iota(jnp.int32, (8, LANES), 0)
    if j >= 10:
        return [cells[v ^ (1 << (j - 10))] for v in range(len(cells))]
    axis, size, place, bit = (1, LANES, lane, 1 << j) if j < 7 else (0, 8, sub, 1 << (j - 7))
    if 2 * bit == size:
        return [roll(c, bit, axis) for c in cells]
    upper = (place & bit) != 0
    return [jnp.where(upper, roll(c, bit, axis), roll(c, size - bit, axis)) for c in cells]


def stages_of(count):
    return 10 + count.bit_length() - 1


def routes(wet):
    count = len(wet)
    flags = jnp.concatenate([jnp.where(w, 1.0, 0.0) for w in wet], axis=0)
    height = flags.shape[0]
    upper = lax.broadcasted_iota(jnp.int32, (LANES, LANES), 0) <= lax.broadcasted_iota(jnp.int32, (LANES, LANES), 1)
    lower = lax.broadcasted_iota(jnp.int32, (height, height), 1) < lax.broadcasted_iota(jnp.int32, (height, height), 0)
    upto = jnp.dot(flags, jnp.where(upper, 1.0, 0.0), preferred_element_type=jnp.float32)
    totals = jnp.broadcast_to(upto[:, LANES - 1:], (height, LANES))
    before = jnp.dot(jnp.where(lower, 1.0, 0.0), totals, preferred_element_type=jnp.float32)
    rank = jnp.where(flags > 0.0, (before + upto - flags).astype(jnp.int32), -1)
    ranks = [rank[8 * v:8 * v + 8] for v in range(count)]
    lane = lax.broadcasted_iota(jnp.int32, (8, LANES), 1)
    sub = lax.broadcasted_iota(jnp.int32, (8, LANES), 0)
    packing = [jnp.zeros((8, LANES), jnp.int32)] * count
    unpacking = [jnp.zeros((8, LANES), jnp.int32)] * count
    for j in range(stages_of(count)):
        others = swapped(ranks, j)
        following = []
        for v in range(count):
            here = (lane >> j) & 1 if j < 7 else (sub >> (j - 7)) & 1 if j < 10 else (v >> (j - 10)) & 1
            mine, other = ranks[v], others[v]
            takes = jnp.where(other >= 0, ((other >> j) & 1) ^ here, 1) == 0
            stays = jnp.where(mine >= 0, ((mine >> j) & 1) ^ here, 1) == 0
            leaves = jnp.where(mine >= 0, ((mine >> j) & 1) ^ here, 0) == 1
            packing[v] = jnp.where(takes, packing[v] | (1 << j), packing[v])
            unpacking[v] = jnp.where(leaves, unpacking[v] | (1 << j), unpacking[v])
            following.append(jnp.where(takes, other, jnp.where(stays, mine, -1)))
        ranks = following
    return packing, unpacking


def moved(layers, masks, order):
    for j in order:
        takes = [(mask & (1 << j)) != 0 for mask in masks]
        layers = [
            [jnp.where(t, o, c) for t, o, c in zip(takes, swapped(cells, j), cells)] for cells in layers
        ]
    return layers


def pieces(block):
    tall, wide = block.shape
    return [
        block[r:r + 8, c:c + LANES] for r in range(0, tall, 8) for c in range(0, wide, LANES)
    ]


def exchange(
    ny, nx, groups,
    warmth_ref, salt_ref, tally_ref,
    tile_ref, bottom_ref, sides_ref, north_ref, south_ref, fold_ref,
    warmth, salt, tally, dens, pack, outbox, inbox, packing, unpacking, low, high,
    load_sem, send_sem, recv_sem, bsend_sem, brecv_sem, psend_sem, precv_sem, own_sem, hsend_sem, hrecv_sem,
):
    y, x = lax.axis_index("ty"), lax.axis_index("tx")
    levels, band, width = dens.shape
    wide = width // nx
    depth = levels // groups
    up, down = lax.rem(y + 1, ny), lax.rem(y + ny - 1, ny)
    last = y == ny - 1

    loads = []
    for g in range(groups):
        part = pl.ds(g * depth, depth)
        pair = [
            pltpu.make_async_copy(warmth_ref.at[part], warmth.at[part], load_sem.at[2 * g]),
            pltpu.make_async_copy(salt_ref.at[part], salt.at[part], load_sem.at[2 * g + 1]),
        ]
        if g == 0:
            load_tally = pltpu.make_async_copy(tally_ref, tally, load_sem.at[2 * groups])
            load_tally.start()
        for copy in pair:
            copy.start()
        loads.append(pair)

    barrier = pltpu.get_barrier_semaphore()
    for m in range(1, nx):
        pl.semaphore_signal(barrier, inc=1, device_id=(y, x ^ m), device_id_type=MESH)
    for other in (up, down):
        pl.semaphore_signal(barrier, inc=1, device_id=(other, x), device_id_type=MESH)

    def columns(t):
        return pl.ds(pl.multiple_of(t * wide, LANES), wide)

    def rows(t):
        return pl.ds(pl.multiple_of(t * band, 8), band)

    mine = rows(x)

    def bottom_copy(m):
        t = x ^ m
        return pltpu.make_async_remote_copy(
            src_ref=tally_ref.at[:, columns(t)], dst_ref=bottom_ref.at[mine],
            send_sem=bsend_sem.at[m], recv_sem=brecv_sem.at[x], device_id=(y, t), device_id_type=MESH)

    def dens_copy(g, m):
        t = x ^ m
        part = pl.ds(g * depth, depth)
        return pltpu.make_async_remote_copy(
            src_ref=outbox.at[t, part], dst_ref=inbox.at[x, part],
            send_sem=send_sem.at[g, m], recv_sem=recv_sem.at[g, x], device_id=(y, t), device_id_type=MESH)

    def pack_copy(m):
        t = x ^ m
        return pltpu.make_async_remote_copy(
            src_ref=pack.at[t], dst_ref=sides_ref.at[mine],
            send_sem=psend_sem.at[m], recv_sem=precv_sem.at[x], device_id=(y, t), device_id_type=MESH)

    own = [
        pltpu.make_async_copy(dens.at[:, :, columns(x)], tile_ref.at[:, mine], own_sem.at[0]),
        pltpu.make_async_copy(tally_ref.at[:, columns(x)], bottom_ref.at[mine], own_sem.at[1]),
        pltpu.make_async_copy(pack.at[x], sides_ref.at[mine], own_sem.at[2]),
    ]
    far = [m for m in range(nx - 1, 0, -1) if m >= nx // 2]
    near = [m for m in range(nx - 1, 0, -1) if m < nx // 2]

    def level(k, _):
        height = 5.0 + 10.0 * k.astype(jnp.float32)

        def block(t, _):
            cols = columns(t)
            value = density(warmth[k, :, cols], salt[k, :, cols], k < tally[:, cols], height)
            dens[k, :, cols] = value
            return 0

        lax.fori_loop(0, nx, block, 0)
        return 0

    load_tally.wait()
    for copy in loads[0]:
        copy.wait()
    lax.fori_loop(0, depth, level, 0)
    pl.semaphore_wait(barrier, nx - 1 + 2)
    for m in far + near:
        bottom_copy(m).start()
    own[1].start()

    lane = lax.broadcasted_iota(jnp.int32, (band, LANES), 1)

    def fill(t, _):
        before = lax.rem(t + nx - 1, nx)
        after = lax.rem(t + 1, nx)
        left = tally[:, pl.ds(pl.multiple_of(before * wide + wide - LANES, LANES), LANES)].astype(jnp.float32)
        right = tally[:, pl.ds(pl.multiple_of(after * wide, LANES), LANES)].astype(jnp.float32)
        cells = jnp.where(lane == 2 * levels, jnp.broadcast_to(left[:, LANES - 1:], (band, LANES)), 0.0)
        cells = jnp.where(lane == 2 * levels + 1, jnp.broadcast_to(right[:, :1], (band, LANES)), cells)
        pack[t] = cells
        return 0

    count = band * wide // (8 * LANES)
    kept = outbox.shape[2] // 8
    stages = stages_of(count)

    def plan(m, _):
        t = x ^ m
        wet = [piece > 0 for piece in pieces(tally[:, columns(t)])]
        for v, mask in enumerate(routes(wet)[0]):
            packing[t, v] = mask
        return 0

    def gather(g, first):
        def block(i, _):
            t = x ^ (first - i)
            masks = [packing[t, v] for v in range(count)]
            for k0 in range(0, depth, 2):
                ks = [g * depth + k for k in range(k0, min(k0 + 2, depth))]
                layers = moved([pieces(dens[k, :, columns(t)]) for k in ks], masks, range(stages))
                for k, cells in zip(ks, layers):
                    for v in range(kept):
                        outbox[t, k, 8 * v:8 * v + 8, :] = cells[v]
            return 0
        return block

    lax.fori_loop(nx // 2, nx, plan, 0)

    for g in range(groups):
        if g > 0:
            for copy in loads[g]:
                copy.wait()
            lax.fori_loop(g * depth, (g + 1) * depth, level, 0)
        lax.fori_loop(0, len(far), gather(g, far[0]), 0)
        for m in far:
            dens_copy(g, m).start()
        if g == 0:
            lax.fori_loop(1, nx // 2, plan, 0)
        lax.fori_loop(0, len(near), gather(g, near[0]), 0)
    lax.fori_loop(0, nx, fill, 0)

    def edges(t, _):
        before = lax.rem(t + nx - 1, nx)
        after = lax.rem(t + 1, nx)
        before_cols = pl.ds(pl.multiple_of(before * wide + wide - LANES, LANES), LANES)
        after_cols = pl.ds(pl.multiple_of(after * wide, LANES), LANES)
        cells = pack[t]
        for k in range(levels):
            left = jnp.broadcast_to(dens[k, :, before_cols][:, LANES - 1:], (band, LANES))
            right = jnp.broadcast_to(dens[k, :, after_cols][:, :1], (band, LANES))
            cells = jnp.where(lane == k, left, jnp.where(lane == levels + k, right, cells))
        pack[t] = cells
        return 0

    lax.fori_loop(0, nx, edges, 0)
    own[0].start()
    own[2].start()
    for g in range(groups):
        for m in near:
            dens_copy(g, m).start()
    for m in far + near:
        pack_copy(m).start()

    own[0].wait()
    own[1].wait()
    for m in far + near:
        bottom_copy(m).wait_send()
    for s in range(nx):
        @pl.when(x != s)
        def _():
            pltpu.make_async_copy(bottom_ref.at[rows(s)], bottom_ref.at[rows(s)], brecv_sem.at[s]).wait()

    def unplan(m, _):
        s = x ^ m
        wet = [piece > 0 for piece in pieces(bottom_ref[rows(s), :])]
        for v, mask in enumerate(routes(wet)[1]):
            unpacking[s, v] = mask
        return 0

    lax.fori_loop(1, nx, unplan, 0)

    def spread(first, number):
        def block(q, _):
            g, s = q // number, x ^ (first - q % number)
            part = inbox.at[s, pl.ds(g * depth, depth)]
            pltpu.make_async_copy(part, part, recv_sem.at[g, s]).wait()
            masks = [unpacking[s, v] for v in range(count)]
            blank = [jnp.zeros((8, LANES), jnp.float32)] * (count - kept)
            for k0 in range(0, depth, 2):
                ks = [g * depth + k for k in range(k0, min(k0 + 2, depth))]
                layers = [[inbox[s, k, 8 * v:8 * v + 8, :] for v in range(kept)] + blank for k in ks]
                layers = moved(layers, masks, range(stages - 1, -1, -1))
                for k, cells in zip(ks, layers):
                    for r in range(0, band, 8):
                        line = r // 8 * (wide // LANES)
                        value = jnp.concatenate(cells[line:line + wide // LANES], axis=1)
                        at = pl.ds(pl.multiple_of(s * band + r, 8), 8)
                        tile_ref[k, at, :] = jnp.where(k < bottom_ref[at, :], value, 0.0)
            return 0
        return block

    lax.fori_loop(0, groups * len(far), spread(far[0], len(far)), 0)
    lax.fori_loop(0, groups * len(near), spread(near[0], len(near)), 0)
    tall = nx * band
    for k in range(levels):
        low[k:k + 1, :] = tile_ref[k, 0:1, :]
        high[k:k + 1, :] = tile_ref[k, tall - 1:tall, :]
    low[levels:, :] = jnp.broadcast_to(bottom_ref[0:1, :].astype(jnp.float32), (8, wide))
    high[levels:, :] = jnp.broadcast_to(bottom_ref[tall - 1:tall, :].astype(jnp.float32), (8, wide))

    def halo(index, src, dst, target):
        return pltpu.make_async_remote_copy(
            src_ref=src, dst_ref=dst, send_sem=hsend_sem.at[index], recv_sem=hrecv_sem.at[index],
            device_id=target, device_id_type=MESH)

    to_south = halo(0, low, north_ref, (down, x))
    to_north = halo(1, high, south_ref, (up, x))
    across = halo(2, high, fold_ref, (y, x ^ (nx - 1)))
    to_south.start()
    to_north.start()

    @pl.when(last)
    def _():
        across.start()

    for s in range(nx):
        @pl.when(x != s)
        def _():
            pltpu.make_async_copy(sides_ref.at[rows(s)], sides_ref.at[rows(s)], precv_sem.at[s]).wait()
    own[2].wait()
    to_south.wait()
    to_north.wait()

    @pl.when(last)
    def _():
        across.wait()

    for m in far + near:
        pack_copy(m).wait_send()
        for g in range(groups):
            dens_copy(g, m).wait_send()


def stencil(
    ny, levels, per,
    tile_ref, bottom_ref, sides_ref, north_ref, south_ref, fold_ref,
    dens_ref, lap_ref,
    north, south, bottoms,
):
    y = lax.axis_index("ty")
    tall, wide = bottom_ref.shape
    row = lax.broadcasted_iota(jnp.int32, (tall, wide), 0)
    col = lax.broadcasted_iota(jnp.int32, (tall, wide), 1)
    side_lane = lax.broadcasted_iota(jnp.int32, sides_ref.shape, 1)

    def side(index):
        return jnp.sum(jnp.where(side_lane == index, sides_ref[...], 0.0), axis=1, keepdims=True)

    def around(cells, top, base, left, right):
        above = jnp.where(row == tall - 1, top, pltpu.roll(cells, tall - 1, 0))
        below = jnp.where(row == 0, base, pltpu.roll(cells, 1, 0))
        east = jnp.where(col == wide - 1, right, pltpu.roll(cells, wide - 1, 1))
        west = jnp.where(col == 0, left, pltpu.roll(cells, 1, 1))
        return above, below, east, west

    @pl.when(pl.program_id(0) == 0)
    def _():
        mirror = fold_ref[...]
        lane = lax.broadcasted_iota(jnp.int32, mirror.shape, 1)
        bit = 1
        while bit < wide:
            mirror = jnp.where((lane & bit) != 0, pltpu.roll(mirror, bit, 1), pltpu.roll(mirror, wide - bit, 1))
            bit *= 2
        north[...] = jnp.where(y == ny - 1, mirror, north_ref[...])
        south[...] = jnp.where(y == 0, 0.0, south_ref[...])
        own = bottom_ref[...].astype(jnp.float32)
        near = around(own, north[levels:levels + 1, :], south[levels:levels + 1, :], side(2 * levels), side(2 * levels + 1))
        bottoms[0] = own
        for index in range(4):
            bottoms[index + 1] = near[index]

    for j in range(per):
        k = pl.program_id(0) * per + j
        number = k.astype(jnp.float32)
        cells = tile_ref[j]
        near = around(cells, north[pl.ds(k, 1), :], south[pl.ds(k, 1), :], side(k), side(levels + k))
        count = jnp.where(number < bottoms[1], 1.0, 0.0)
        for index in range(2, 5):
            count = count + jnp.where(number < bottoms[index], 1.0, 0.0)
        total = (near[0] + near[1]) + (near[2] + near[3]) - count * cells
        dens_ref[j] = cells
        lap_ref[j] = jnp.where(number < bottoms[0], total, 0.0)


def on_device(ny, nx, potential_warmth, saltiness_field, ocean_tier_tally):
    levels, band, width = potential_warmth.shape
    wide, tall = width // nx, band * nx
    groups = 4 if levels % 4 == 0 else 1
    count = band * wide // (8 * LANES)
    kept = 8 * (3 * count // 4)
    hbm = pl.BlockSpec(memory_space=pltpu.HBM)
    vmem = pl.BlockSpec(memory_space=pltpu.VMEM)
    f32, i32 = jnp.float32, jnp.int32
    edge = jax.ShapeDtypeStruct((levels + 8, wide), f32)
    dma = pltpu.SemaphoreType.DMA
    parts = pl.pallas_call(
        functools.partial(exchange, ny, nx, groups),
        out_shape=(
            jax.ShapeDtypeStruct((levels, tall, wide), f32),
            jax.ShapeDtypeStruct((tall, wide), i32),
            jax.ShapeDtypeStruct((tall, LANES), f32),
            edge, edge, edge,
        ),
        in_specs=[hbm] * 3,
        out_specs=(vmem,) * 6,
        scratch_shapes=[
            pltpu.VMEM((levels, band, width), f32),
            pltpu.VMEM((levels, band, width), f32),
            pltpu.VMEM((band, width), i32),
            pltpu.VMEM((levels, band, width), f32),
            pltpu.VMEM((nx, band, LANES), f32),
            pltpu.VMEM((nx, levels, kept, LANES), f32),
            pltpu.VMEM((nx, levels, kept, LANES), f32),
            pltpu.VMEM((nx, count, 8, LANES), i32),
            pltpu.VMEM((nx, count, 8, LANES), i32),
            pltpu.VMEM((levels + 8, wide), f32),
            pltpu.VMEM((levels + 8, wide), f32),
            dma((2 * groups + 1,)),
            dma((groups, nx)), dma((groups, nx)),
            dma((nx,)), dma((nx,)), dma((nx,)), dma((nx,)),
            dma((3,)), dma((3,)), dma((3,)),
        ],
        compiler_params=pltpu.CompilerParams(collective_id=0, has_side_effects=True, vmem_limit_bytes=GRANT),
        cost_estimate=pl.CostEstimate(flops=0, bytes_accessed=16 * levels * band * width, transcendentals=0),
        name="exchange",
    )(potential_warmth, saltiness_field, ocean_tier_tally)
    per = 2 if levels % 2 == 0 else 1
    block = pl.BlockSpec((per, tall, wide), lambda i: (i, 0, 0))
    whole = pl.BlockSpec(memory_space=pltpu.VMEM)
    out = jax.ShapeDtypeStruct((levels, tall, wide), f32)
    return pl.pallas_call(
        functools.partial(stencil, ny, levels, per),
        grid=(levels // per,),
        out_shape=(out, out),
        in_specs=[block] + [whole] * 5,
        out_specs=(block, block),
        scratch_shapes=[
            pltpu.VMEM((levels + 8, wide), f32),
            pltpu.VMEM((levels + 8, wide), f32),
            pltpu.VMEM((5, tall, wide), f32),
        ],
        compiler_params=pltpu.CompilerParams(vmem_limit_bytes=24 * MIB),
        name="stencil",
    )(*parts)


def solution(mesh):
    placed = (P(None, ("ty", "tx"), None), P(None, ("ty", "tx"), None), P(("ty", "tx"), None))
    return jax.shard_map(
        functools.partial(on_device, mesh.shape["ty"], mesh.shape["tx"]),
        mesh=mesh,
        in_specs=placed,
        out_specs=(P(None, "ty", "tx"), P(None, "ty", "tx")),
        check_vma=False,
    )
```
